256 devices in a mesh: groups: 2 (over y), dp: 16 (over z), section: 4 (over x), tensor: 2 (over core).
Axes of the slice: x: 4, y: 2, z: 16, core: 2. Of those that a mesh axis runs over, the one named last changes fastest.
The devices are a block of a 4x16x16 slice.
Arguments:
- hidden: bfloat16 [512, 8, 5120], P(('groups', 'dp')), parts along dimension 0, may hold values from -6 to 6
- unembed: bfloat16 [512, 8, 5120], P(('groups', 'dp')), parts along dimension 0, may hold values from -0.02734375 to 0.02734375
- value_proj: bfloat16 [4, 5120, 512], P('section', 'dp', 'tensor'), may hold values from -0.078125 to 0.078125
- output_proj: bfloat16 [4, 512, 5120], P('section', 'tensor', 'dp'), may hold values from -0.125 to 0.125
- norm_gains: float32 [4, 5120], P('section'), may hold values from 0.1 to 1.9
- survive: int32 [32], P(('groups', 'dp')), parts along dimension 0, may hold values from 0 to 1, as said below
- lengths: int32 [512], P(('groups', 'dp')), parts along dimension 0, may hold values from 1 to 8
- assign: int32 [512], P(('groups', 'dp')), parts along dimension 0, may hold values from 0 to 16, as said below
- advantage: float32 [512], P(('groups', 'dp')), parts along dimension 0, may hold values from -4 to 4
- reference_logit: float32 [512, 8], P(('groups', 'dp')), parts along dimension 0, may hold values from -4 to 4
- recorded_gap: float32 [512, 8], P(('groups', 'dp')), parts along dimension 0, may hold values from -2 to 2
Outputs:
- grad_value: float32 [8, 5120, 512], P(('groups', 'section'), 'dp', 'tensor'), parts along dimension 0
- grad_output: float32 [8, 512, 5120], P(('groups', 'section'), 'tensor', 'dp'), parts along dimension 0
The draws below stay inside these ranges and needn't reach their ends.
There are 2 independent parts, one for each index of `groups`. The reference program is written for one: setup_inputs(seed, part) draws one part's arguments, and reference() takes and returns one part's arrays. A program takes and returns all parts, laid end to end along the dimension named above; an argument that names none is the same for every part. Nothing has to cross between parts.
Inputs may be any that keep to these rules, and one draw needn't show every extreme that they name: `survive`: 1 where the group of 16 responses is kept, 0 where it is dropped; in every draw all groups of some dp index are kept. `assign`: the 16 slots of a dp index list the local positions (0 to 15) of the responses of its kept groups, each exactly once, then hold 16 in every other slot.
All inputs are finite; a program needn't handle non-finite values.
Results may differ from the reference program's by a relative error of at most 0.029.
Values may be sent and summed in bfloat16 or wider, within the bound.
A program may use at most 64 MiB of HBM per device.

```python
import math
import jax
import jax.numpy as jnp
from jax import lax

D = 5120
VALUE_W = 512
GROUP = 16
GROUPS_DEV = 1
LMAX = 8
LAYERS = 4
RESP_DEV = 16
RESPONSES = 256
GROUPS = 16
N_DP = 16
N_TENSOR = 2


def survival_plan(key):
    base = jax.random.fold_in(key, 17)
    roll_key, force_key, order_key = jax.random.split(base, 3)
    device = jnp.arange(GROUPS, dtype=jnp.int32) // GROUPS_DEV
    threshold = 300 + 700 * device // max(N_DP - 1, 1)
    survival_roll = jax.random.randint(roll_key, (GROUPS,), 0, 1000)
    forced = jax.random.randint(force_key, (), 0, N_DP)
    alive_mask = ((survival_roll < threshold) | (device == forced)).astype(jnp.int32)
    return (alive_mask, order_key)


def draw_survive(key, part):
    alive_mask, order_key = survival_plan(key)
    return alive_mask


def draw_assign(key, part):
    alive_mask, order_key = survival_plan(key)
    per_device = jnp.repeat(alive_mask, GROUP).reshape(N_DP, RESP_DEV)
    subkeys = jax.random.split(order_key, N_DP)
    priority = jax.vmap(lambda subkey: jax.random.permutation(subkey, RESP_DEV))(subkeys).astype(jnp.int32)
    sort_key = (1 - per_device) * RESP_DEV + priority
    slot_order = jnp.argsort(sort_key, axis=1, stable=True).astype(jnp.int32)
    alive_count = jnp.sum(per_device, axis=1, keepdims=True)
    slot_index = lax.broadcasted_iota(jnp.int32, (N_DP, RESP_DEV), 1)
    return jnp.where(slot_index < alive_count, slot_order, RESP_DEV).astype(jnp.int32).reshape(RESPONSES)


def set_ends(drawn, rng, low, high):
    extent = drawn.shape
    spot = [jax.random.randint(jax.random.fold_in(rng, axis), (), 0, extent[axis]) for axis in range(len(extent))]
    drawn = drawn.at[tuple(spot)].set(low)
    longest = extent.index(max(extent))
    spot[longest] = (spot[longest] + 1) % extent[longest]
    return drawn.at[tuple(spot)].set(high)


def with_spikes(values, rng, source, target, parts, factor):
    owner, partner = [(jnp.arange(values.shape[axis_at]) // (values.shape[axis_at] // parts)).reshape([-1 if axis == axis_at else 1 for axis in range(values.ndim)]) for axis_at in (source, target)]
    chosen = jax.random.permutation(rng, parts)[partner]
    strong = (owner == chosen) | (owner == (partner + parts // 2) % parts)
    return jnp.where(strong, factor * values, values)


def shard_levels(own_key, shape, cuts, least, top_value):
    gain, own = 1.0, jax.random.fold_in(own_key, 6)
    for position, parts in cuts:
        heights = jnp.exp(jax.random.uniform(jax.random.fold_in(own, position), (parts,), jnp.float32, least / len(cuts), top_value / len(cuts)))
        gain = gain * jnp.repeat(heights, shape[position] // parts).reshape([-1 if axis == position else 1 for axis in range(len(shape))])
    return gain


def normal_values(own_key, dims, scale, limit, cuts=(), held_as=jnp.bfloat16):
    result = jax.random.normal(own_key, dims, jnp.float32) * scale
    if len(cuts) > 0:
        result = shard_levels(own_key, dims, cuts, -0.22, 0.18) * result
    return jnp.clip(result, min=-limit, max=limit).astype(held_as)


def heavy_noise(key, shape, scale, most, cuts, heavy, held_as=jnp.bfloat16):
    entries = scale * jax.random.normal(key, shape, jnp.float32)
    if cuts:
        entries = entries * shard_levels(key, shape, cuts, -0.22, 0.18)
    return jnp.clip(with_spikes(entries, jax.random.fold_in(key, 3), *heavy), -most, most).astype(held_as)


def setup_inputs(seed: int = 0, part: int = 0) -> dict:
    key_list = jax.random.split(jax.random.key(seed), 12)
    own_keys = jax.random.split(jax.random.fold_in(key_list[11], part), 12)
    return {
        "hidden": heavy_noise(own_keys[0], (RESPONSES, LMAX, D), 1.0, 6.0, ((0, 16),), (0, 2, 16, 2.0)),
        "unembed": normal_values(own_keys[1], (RESPONSES, LMAX, D), (10 * D) ** -0.5, 0.02734375, ((0, 16),)),
        "value_proj": normal_values(key_list[2], (LAYERS, D, VALUE_W), D ** -0.5, 0.078125, ((0, 4), (1, 16), (2, 2))),
        "output_proj": normal_values(key_list[3], (LAYERS, VALUE_W, D), (4 * VALUE_W) ** -0.5, 0.125, ((0, 4), (1, 2), (2, 16))),
        "norm_gains": jnp.clip(1.0 + 0.18 * jax.random.normal(key_list[4], (LAYERS, D), jnp.float32), 0.1, 1.9),
        "survive": draw_survive(jax.random.fold_in(jax.random.fold_in(key_list[11], part), 71), part),
        "lengths": set_ends(jax.random.randint(own_keys[6], (RESPONSES,), 1, LMAX + 1), jax.random.fold_in(own_keys[6], 1), 1, LMAX).astype(jnp.int32),
        "assign": draw_assign(jax.random.fold_in(jax.random.fold_in(key_list[11], part), 71), part),
        "advantage": normal_values(own_keys[8], (RESPONSES,), 1.0, 4.0, ((0, 16),), jnp.float32),
        "reference_logit": normal_values(own_keys[9], (RESPONSES, LMAX), 0.7, 4.0, ((0, 16),), jnp.float32),
        "recorded_gap": normal_values(own_keys[10], (RESPONSES, LMAX), 0.3, 2.0, ((0, 16),), jnp.float32),
    }


eps_norm = 1e-06
loss_scale = 4096.0
clip_high = math.log(1.28)
clip_low = math.log(0.8)

def norm_forward(row_block, norm_gain):
    values = row_block.astype(jnp.float32)
    inverse = lax.rsqrt(lax.optimization_barrier(jnp.mean(values * values, axis=-1, keepdims=True)) + eps_norm)
    return (values, inverse, (values * inverse * norm_gain).astype(jnp.bfloat16))

def norm_backward(values, inverse, norm_gain, upstream):
    scaled = upstream * norm_gain
    inner_sum = lax.optimization_barrier(jnp.sum(scaled * values, axis=-1, keepdims=True)) / values.shape[-1]
    return inverse * scaled - values * (inverse * inverse * inverse) * inner_sum

def contract_last(left_rows, right_rows):
    return lax.dot_general(left_rows, right_rows, (((1,), (1,)), ((), ())), preferred_element_type=jnp.float32)

def rounded(partial_piece):
    return lax.optimization_barrier(partial_piece.astype(jnp.bfloat16)).astype(jnp.float32)

def reference(hidden, unembed, value_proj, output_proj, norm_gains, survive, lengths, assign, advantage, reference_logit, recorded_gap):
    owner_index = jnp.arange(RESPONSES, dtype=jnp.int32) // RESP_DEV
    chosen = jnp.where(assign >= RESP_DEV, RESPONSES, assign + owner_index * RESP_DEV).astype(jnp.int32)

    def pick(array):
        return jnp.take(array, chosen, axis=0, mode='fill', fill_value=0)
    row_count = RESPONSES * LMAX
    block_width = VALUE_W // N_TENSOR
    current = pick(hidden).reshape(row_count, D)
    unembed_rows = pick(unembed).reshape(row_count, D).astype(jnp.float32)
    positions = lax.broadcasted_iota(jnp.int32, (RESPONSES, LMAX), 1)
    live_mask = (positions < pick(lengths)[:, None]).astype(jnp.float32)
    advantages = jnp.broadcast_to(pick(advantage)[:, None], (RESPONSES, LMAX))
    gap_rows = pick(recorded_gap)
    clipped = (advantages > 0) & (gap_rows > clip_high) | (advantages < 0) & (gap_rows < clip_low)
    kept_mask = 1.0 - clipped.astype(jnp.float32)
    alive_mask = jnp.repeat(survive, GROUP)
    token_count = jnp.sum((alive_mask * lengths).astype(jnp.float32))
    weight_rows = (-loss_scale * advantages * kept_mask * live_mask).reshape(row_count)
    logit_base = pick(reference_logit).reshape(row_count)
    saved = []
    for layer_index in range(LAYERS):
        values, inverse, normed = norm_forward(current, norm_gains[layer_index])
        projected = jnp.dot(normed, value_proj[layer_index], preferred_element_type=jnp.float32).astype(jnp.bfloat16)
        mixed_sum = jnp.zeros((row_count, D), jnp.float32)
        for tensor_part in range(N_TENSOR):
            low = tensor_part * block_width
            partial_piece = jnp.dot(projected[:, low:low + block_width], output_proj[layer_index, low:low + block_width, :], preferred_element_type=jnp.float32)
            mixed_sum = mixed_sum + rounded(partial_piece)
        saved.append((current, normed, projected))
        current = (values + mixed_sum).astype(jnp.bfloat16)
    top_rows = current.astype(jnp.float32)
    logit = lax.optimization_barrier(jnp.sum(top_rows * unembed_rows, axis=-1))
    seed_rows = weight_rows * jnp.exp(logit - logit_base)
    upstream = (seed_rows[:, None] * unembed_rows).astype(jnp.bfloat16)
    grads_value = [None] * LAYERS
    grads_output = [None] * LAYERS
    for layer_index in reversed(range(LAYERS)):
        entering, normed, projected = saved[layer_index]
        grad_projected = contract_last(upstream, output_proj[layer_index]).astype(jnp.bfloat16)
        grad_normed = jnp.zeros((row_count, D), jnp.float32)
        for tensor_part in range(N_TENSOR):
            low = tensor_part * block_width
            partial_piece = contract_last(grad_projected[:, low:low + block_width], value_proj[layer_index][:, low:low + block_width])
            grad_normed = grad_normed + rounded(partial_piece)
        grads_value[layer_index] = jnp.dot(normed.T, grad_projected, preferred_element_type=jnp.float32) / token_count
        grads_output[layer_index] = jnp.dot(projected.T, upstream, preferred_element_type=jnp.float32) / token_count
        values, inverse, unused_normed = norm_forward(entering, norm_gains[layer_index])
        upstream = (upstream.astype(jnp.float32) + norm_backward(values, inverse, norm_gains[layer_index], grad_normed)).astype(jnp.bfloat16)
    return (jnp.stack(grads_value), jnp.stack(grads_output))
```

```python
import functools
import math

import jax
import jax.numpy as jnp
from jax import lax
from jax.experimental import pallas as pl
from jax.experimental.pallas import tpu as pltpu
from jax.sharding import PartitionSpec as P

GROUP = 16

eps_norm = 1e-06
loss_scale = 4096.0
clip_high = math.log(1.28)
clip_low = math.log(0.8)

F32 = jnp.float32
BF16 = jnp.bfloat16
MESH = pl.DeviceIdType.MESH


def dot_nn(a, b):
    return jnp.dot(a, b, preferred_element_type=F32)


def dot_nt(a, b):
    return lax.dot_general(a, b, (((1,), (1,)), ((), ())), preferred_element_type=F32)


def dot_tn(a, b):
    return lax.dot_general(a, b, (((0,), (0,)), ((), ())), preferred_element_type=F32)


def kernel(
    dims,
    hid, une, wown, gown, rowd, tgt,
    out,
    wfull, gall, cnts, xs, us, projs, rcols, gcur, wg, rbu, rbd, obuf, osrc,
    arsrc, arbuf, stsrc, stbuf, dsrc, dbuf, tsrc, tbuf,
    xa_s, xa_r, ga_s, ga_r, ag_s, ag_r, cn_s, cn_r, ar_s, ar_r, st_s, st_r,
    d_s, d_r, t_s, t_r, rs_s, rs_r, o_s, o_r,
):
    n, ns, rows, sub, half, width = dims
    q = n * sub
    layers = ns
    j = lax.axis_index("dp")
    s = lax.axis_index("section")
    t = lax.axis_index("tensor")
    up, down, other = lax.rem(j + 1, n), lax.rem(j + n - 1, n), 1 - t
    pending = []

    def remote(src, dst, send, recv, device):
        return pltpu.make_async_remote_copy(
            src_ref=src, dst_ref=dst, send_sem=send, recv_sem=recv,
            device_id=device, device_id_type=MESH,
        )

    def go(*args):
        copy = remote(*args)
        copy.start()
        pending.append(copy)
        return copy

    def block(offset):
        return lax.rem(j + n + offset, n)

    barrier = pltpu.get_barrier_semaphore()
    peers = [{"dp": up}, {"dp": down}, {"tensor": other}]
    peers += [{"section": lax.rem(s + k, ns)} for k in range(1, ns)]
    for peer in peers:
        pl.semaphore_signal(barrier, inc=1, device_id=peer, device_id_type=MESH)
    pl.semaphore_wait(barrier, len(peers))

    for k in range(1, ns):
        to = lax.rem(s + k, ns)
        go(wown.at[to], wfull.at[s, j], xa_s.at[k - 1], xa_r.at[s], {"section": to})
        go(gown.at[to], gall.at[s], ga_s.at[k - 1], ga_r.at[s], {"section": to})
    wfull[s, j] = wown[s]
    gall[s] = gown[s]
    cnts[j] = jnp.broadcast_to(rowd[3:4, :], cnts.shape[1:])

    def layer_arrived(l):
        @pl.when(s != l)
        def _():
            away = {"section": lax.rem(s + 1, ns)}
            remote(wown.at[0], wfull.at[l, j], xa_s.at[0], xa_r.at[l], away).wait_recv()
            remote(gown.at[0], gall.at[l], ga_s.at[0], ga_r.at[l], away).wait_recv()

    steps = n // 2

    def reach(l, way):
        return steps if (l + way) % 2 == 0 else steps - 1

    toward = [{"dp": up}, {"dp": down}]
    sign = [1, -1]

    def ag_send(l, k, way):
        if k <= reach(l, way):
            b = block(-sign[way] * (k - 1))
            go(wfull.at[l, b], wfull.at[l, b], ag_s.at[l, way, k - 1], ag_r.at[l, way, k - 1], toward[way])
            if l == 0:
                go(cnts.at[b], cnts.at[b], cn_s.at[way, k - 1], cn_r.at[way, k - 1], toward[way])

    def ag_recv(l, k, way):
        if k <= reach(l, way):
            b = block(-sign[way] * k)
            remote(wfull.at[l, b], wfull.at[l, b], ag_s.at[l, way, k - 1], ag_r.at[l, way, k - 1], toward[way]).wait_recv()
            if l == 0:
                remote(cnts.at[b], cnts.at[b], cn_s.at[way, k - 1], cn_r.at[way, k - 1], toward[way]).wait_recv()

    def ag_tick(ls, k):
        for l in ls:
            for way in range(2):
                ag_recv(l, k, way)
                ag_send(l, k + 1, way)

    eye = lax.broadcasted_iota(jnp.int32, (rows, rows), 0) == lax.broadcasted_iota(jnp.int32, (rows, rows), 1)

    def to_row(column):
        return jnp.sum(jnp.where(eye, column, 0.0), axis=0, keepdims=True)

    def to_col(row):
        return jnp.sum(jnp.where(eye, row, 0.0), axis=1, keepdims=True)

    def weight(l, first):
        w = wfull[l, :, :, 0:half] if first else wfull[l, :, :, half : 2 * half]
        return w.reshape(q, half)

    def gain(l):
        return jnp.concatenate([gall[l, i : i + 1, :] for i in range(q // 128)], axis=1)

    def ar_send(i, value, stats=None):
        arsrc[i] = value
        if stats is not None:
            first = lax.broadcasted_iota(jnp.int32, (8, rows), 0) == 0
            stsrc[i] = jnp.where(first, stats[0], stats[1])
        for k in range(1, ns):
            to = {"section": lax.rem(s + k, ns)}
            if stats is not None:
                go(stsrc.at[i], stbuf.at[i, k - 1], st_s.at[i, k - 1], st_r.at[i, k - 1], to)
            go(arsrc.at[i], arbuf.at[i, k - 1], ar_s.at[i, k - 1], ar_r.at[i, k - 1], to)

    def ar_recv(i, stats=False):
        away = {"section": lax.rem(s + 1, ns)}
        if stats:
            for k in range(1, ns):
                remote(stsrc.at[i], stbuf.at[i, k - 1], st_s.at[i, k - 1], st_r.at[i, k - 1], away).wait_recv()
            both = stsrc[i]
            for k in range(1, ns):
                both = both + stbuf[i, k - 1]
        for k in range(1, ns):
            remote(arsrc.at[i], arbuf.at[i, k - 1], ar_s.at[i, k - 1], ar_r.at[i, k - 1], away).wait_recv()
        total = arsrc[i].astype(F32)
        for k in range(1, ns):
            total = total + arbuf[i, k - 1].astype(F32)
        return (total, both) if stats else total

    def pair_send(i, value):
        dsrc[i] = value
        go(dsrc.at[i], dbuf.at[i], d_s.at[i], d_r.at[i], {"tensor": other})

    def pair_recv(i):
        remote(dsrc.at[i], dbuf.at[i], d_s.at[i], d_r.at[i], {"tensor": other}).wait_recv()
        return dsrc[i].astype(F32) + dbuf[i].astype(F32)

    def small_send(i, column):
        tsrc[i] = jnp.broadcast_to(to_row(column), (8, rows))
        go(tsrc.at[i], tbuf.at[i], t_s.at[i], t_r.at[i], {"tensor": other})

    def small_recv(i):
        remote(tsrc.at[i], tbuf.at[i], t_s.at[i], t_r.at[i], {"tensor": other}).wait_recv()
        return to_col(tsrc[i, 0:1, :] + tbuf[i, 0:1, :])

    def select_features():
        size = tgt.shape[1]
        place = lax.broadcasted_iota(jnp.int32, (size, size), 0)
        for super_index in range(width // (4 * size)):
            total = None
            for c in range(ns):
                pick = (place + c * size == tgt[0:1, :]).astype(F32).astype(BF16)
                at = (super_index * ns + c) * size
                lhs = jnp.concatenate([hid[:, at : at + size], une[:, at : at + size]], axis=0)
                piece = dot_nn(lhs, pick)
                total = piece if total is None else total + piece
            total = total.astype(BF16)
            xs[0, :, super_index * size : (super_index + 1) * size] = total[:rows]
            us[:, super_index * size : (super_index + 1) * size] = total[rows:]

    def contribute(l):
        x = xs[l].astype(F32)
        xg = (x * gain(l)).astype(BF16)
        partial = dot_nn(xg, weight(l, True)).astype(BF16)
        squares = to_row(jnp.sum(x * x, axis=1, keepdims=True))
        inner = squares
        if l == layers - 1:
            inner = to_row(jnp.sum(x * us[...].astype(F32), axis=1, keepdims=True))
        ar_send(l, partial, (squares, inner))

    def collect(l):
        total, both = ar_recv(l, True)
        inverse = lax.rsqrt(to_col(both[0:1, :]) / width + eps_norm)
        rcols[l] = jnp.broadcast_to(inverse, (rows, 128))
        projs[l] = (total * inverse).astype(BF16)
        return both[1:2, :]

    def mix(l):
        pair_send(l, dot_nt(projs[l], weight(l, False)).astype(BF16))

    def advance(l):
        xs[l + 1] = (xs[l].astype(F32) + pair_recv(l)).astype(BF16)

    def early():
        contribute(0)
        yield
        collect(0)
        mix(0)
        yield
        advance(0)
        contribute(1)
        yield
        collect(1)
        mix(1)
        yield
        advance(1)
        yield

    for l in (0, 1):
        layer_arrived(l)
        for way in range(2):
            ag_send(l, 1, way)
    select_features()
    for k in range(1, steps + 1):
        ag_tick((0, 1), k)
        if k == steps:
            for l in (2, 3):
                layer_arrived(l)
                for way in range(2):
                    ag_send(l, 1, way)
    stage = early()
    for k in range(1, steps + 1):
        next(stage, None)
        ag_tick((2, 3), k)
    for _ in stage:
        pass

    contribute(2)
    ar_send(4, dot_nn(us[...], weight(3, False)).astype(BF16))
    collect(2)
    mix(2)
    advance(2)
    contribute(3)
    inner_row = collect(3)
    top = ar_recv(4)
    small_send(3, jnp.sum(projs[3].astype(F32) * top, axis=1, keepdims=True))

    def wgrad(l, gp):
        normed = (xs[l].astype(F32) * rcols[l, :, 0:1] * gain(l)).astype(BF16)
        wg[l, :, :, 0:half] = dot_tn(normed, gp).astype(BF16).reshape(n, sub, half)
        wg[l, :, :, half : 2 * half] = dot_tn(gcur[...], projs[l]).astype(BF16).reshape(n, sub, half)

    landing = [rbu, rbd]

    def rs_send(l, i, way):
        hops = reach(l, way)
        if i <= hops:
            b = block(sign[way] * (hops - i + 1))
            go(wg.at[l, b], landing[way].at[l, i - 1], rs_s.at[l, way, i - 1], rs_r.at[l, way, i - 1], toward[way])

    def rs_recv(l, i, way):
        hops = reach(l, way)
        if i <= hops:
            b = block(sign[way] * (hops - i))
            remote(wg.at[l, b], landing[way].at[l, i - 1], rs_s.at[l, way, i - 1], rs_r.at[l, way, i - 1], toward[way]).wait_recv()
            wg[l, b] = (wg[l, b].astype(F32) + landing[way][l, i - 1].astype(F32)).astype(BF16)

    position = {}

    def rs_start(l):
        for way in range(2):
            rs_send(l, 1, way)
        position[l] = 1

    def rs_tick():
        for l in sorted(position, reverse=True):
            i = position[l]
            if i > steps:
                continue
            for way in range(2):
                rs_recv(l, i, way)
                rs_send(l, i + 1, way)
            position[l] = i + 1
            if i == steps:
                finish(l)

    def finish(l):
        osrc[l] = wg[l, j]

        @pl.when(s == l)
        def _():
            obuf[l] = osrc[l]

        @pl.when(s != l)
        def _():
            remote(osrc.at[l], obuf.at[s], o_s.at[l], o_r.at[s], {"section": l}).start()

    wcol = to_col(rowd[0:1, :])
    base = to_col(rowd[1:2, :])
    held = to_col(rowd[2:3, :])
    inner = to_col(inner_row)
    logit = inner + small_recv(3)
    seed = wcol * jnp.exp(jnp.where(held > 0.0, logit - base, 0.0))
    gp = (seed * top).astype(BF16)
    gcur[...] = (seed * us[...].astype(F32)).astype(BF16)
    for l in range(layers - 1, 0, -1):
        pair_send(2 + l, dot_nt(gp, weight(l, True)).astype(BF16))
        small_send(l - 1, jnp.sum(gp.astype(F32) * projs[l].astype(F32), axis=1, keepdims=True))
        wgrad(l, gp)
        rs_start(l)
        grad_normed = pair_recv(2 + l)
        inverse = rcols[l, :, 0:1]
        inner = small_recv(l - 1) * (inverse * inverse) / width
        gcur[...] = (
            gcur[...].astype(F32) + inverse * gain(l) * grad_normed - xs[l].astype(F32) * inner
        ).astype(BF16)
        ar_send(4 + l, dot_nn(gcur[...], weight(l - 1, False)).astype(BF16))
        rs_tick()
        gp = ar_recv(4 + l).astype(BF16)
    wgrad(0, gp)
    rs_start(0)
    while any(i <= steps for i in position.values()):
        rs_tick()

    for l in range(layers):
        @pl.when(s != l)
        def _():
            remote(osrc.at[l], obuf.at[l], o_s.at[l], o_r.at[l], {"section": l}).wait_send()
            remote(osrc.at[l], obuf.at[l], o_s.at[l], o_r.at[l], {"section": l}).wait_recv()
    tokens = jnp.sum(cnts[:, 0:1, 0:1])
    out[...] = obuf[...].astype(F32) / tokens
    for copy in pending:
        copy.wait_send()


def local(
    hidden,
    unembed,
    value_proj,
    output_proj,
    norm_gains,
    survive,
    lengths,
    assign,
    advantage,
    reference_logit,
    recorded_gap,
):
    resp_count, positions, width = hidden.shape
    own, half = value_proj.shape[1:]
    n, ns = lax.axis_size("dp"), lax.axis_size("section")
    rows = resp_count * positions
    sub = own // ns
    q = n * sub
    section = lax.axis_index("section")

    alive = jnp.repeat(survive, GROUP)
    count = jnp.sum((alive * lengths).astype(F32))
    held = jnp.any(assign[None, :] == jnp.arange(resp_count, dtype=assign.dtype)[:, None], axis=1)
    held = jnp.broadcast_to(held[:, None].astype(F32), (resp_count, positions))
    position = lax.broadcasted_iota(jnp.int32, (resp_count, positions), 1)
    live = (position < lengths[:, None]).astype(F32)
    adv = jnp.broadcast_to(advantage[:, None], (resp_count, positions))
    clipped = (adv > 0) & (recorded_gap > clip_high) | (adv < 0) & (recorded_gap < clip_low)
    kept = 1.0 - clipped.astype(F32)
    weight_rows = -loss_scale * adv * kept * live * held
    rowd = jnp.stack(
        [
            weight_rows.reshape(rows),
            reference_logit.reshape(rows),
            held.reshape(rows),
            jnp.broadcast_to(count, (rows,)),
        ]
        * 2
    )
    wown = jnp.concatenate([value_proj[0], output_proj[0].T], axis=1).reshape(ns, sub, 2 * half)
    gown = norm_gains[0].reshape(n, ns, sub).swapaxes(0, 1).reshape(ns, q // 128, 128)
    size = math.lcm(sub, 128)
    lane = jnp.arange(size, dtype=jnp.int32)
    tgt = jnp.broadcast_to((lane // sub * (ns * sub) + section * sub + lane % sub)[None], (8, size))

    dims = (n, ns, rows, sub, half, width)
    steps = n // 2
    vmem = pl.BlockSpec(memory_space=pltpu.VMEM)
    dma = pltpu.SemaphoreType.DMA
    out = pl.pallas_call(
        functools.partial(kernel, dims),
        out_shape=jax.ShapeDtypeStruct((ns, sub, 2 * half), F32),
        in_specs=[vmem] * 6,
        out_specs=vmem,
        scratch_shapes=[
            pltpu.VMEM((ns, n, sub, 2 * half), BF16),
            pltpu.VMEM((ns, q // 128, 128), F32),
            pltpu.VMEM((n, 8, rows), F32),
            pltpu.VMEM((ns, rows, q), BF16),
            pltpu.VMEM((rows, q), BF16),
            pltpu.VMEM((ns, rows, half), BF16),
            pltpu.VMEM((ns, rows, 128), F32),
            pltpu.VMEM((rows, q), BF16),
            pltpu.VMEM((ns, n, sub, 2 * half), BF16),
            pltpu.VMEM((ns, steps, sub, 2 * half), BF16),
            pltpu.VMEM((ns, steps, sub, 2 * half), BF16),
            pltpu.VMEM((ns, sub, 2 * half), BF16),
            pltpu.VMEM((ns, sub, 2 * half), BF16),
            pltpu.VMEM((8, rows, half), BF16),
            pltpu.VMEM((8, ns - 1, rows, half), BF16),
            pltpu.VMEM((ns, 8, rows), F32),
            pltpu.VMEM((ns, ns - 1, 8, rows), F32),
            pltpu.VMEM((6, rows, q), BF16),
            pltpu.VMEM((6, rows, q), BF16),
            pltpu.VMEM((4, 8, rows), F32),
            pltpu.VMEM((4, 8, rows), F32),
            dma((ns - 1,)), dma((ns,)), dma((ns - 1,)), dma((ns,)),
            dma((ns, 2, steps)), dma((ns, 2, steps)), dma((2, steps)), dma((2, steps)),
            dma((8, ns - 1)), dma((8, ns - 1)), dma((ns, ns - 1)), dma((ns, ns - 1)),
            dma((6,)), dma((6,)), dma((4,)), dma((4,)),
            dma((ns, 2, steps)), dma((ns, 2, steps)), dma((ns,)), dma((ns,)),
        ],
        compiler_params=pltpu.CompilerParams(
            collective_id=0, has_side_effects=True, vmem_limit_bytes=60 * 1024 * 1024
        ),
    )(
        hidden.reshape(rows, width),
        unembed.reshape(rows, width),
        wown,
        gown,
        rowd,
        tgt,
    )
    flat = out.reshape(own, 2 * half)
    return (flat[:, :half][None], flat[:, half:].T[None])


def solution(mesh):
    placed = (
        P(("groups", "dp"), None, None),
        P(("groups", "dp"), None, None),
        P("section", "dp", "tensor"),
        P("section", "tensor", "dp"),
        P("section", None),
        P(("groups", "dp")),
        P(("groups", "dp")),
        P(("groups", "dp")),
        P(("groups", "dp")),
        P(("groups", "dp"), None),
        P(("groups", "dp"), None),
    )
    return jax.shard_map(
        local,
        mesh=mesh,
        in_specs=placed,
        out_specs=(
            P(("groups", "section"), "dp", "tensor"),
            P(("groups", "section"), "tensor", "dp"),
        ),
        check_vma=False,
    )
```

```python
import functools
import math

import jax
import jax.numpy as jnp
from jax import lax
from jax.experimental import pallas as pl
from jax.experimental.pallas import tpu as pltpu
from jax.sharding import PartitionSpec as P

eps_norm = 1e-06
loss_scale = 4096.0
clip_high = math.log(1.28)
clip_low = math.log(0.8)

F32 = jnp.float32
BF16 = jnp.bfloat16
MESH = pl.DeviceIdType.MESH


def dot_nn(a, b):
    return jnp.dot(a, b, preferred_element_type=F32)


def dot_nt(a, b):
    return lax.dot_general(a, b, (((1,), (1,)), ((), ())), preferred_element_type=F32)


def dot_tn(a, b):
    return lax.dot_general(a, b, (((0,), (0,)), ((), ())), preferred_element_type=F32)


def kernel(
    dims,
    hid, une, vown, oown, gown, surv, lens, assign, adv, ref_t, gap_t,
    out,
    xfull, gbuf, wfull, gall, cnts, xs, us, projs, rcols, gcur, wg, rbu, rbd, obuf, osrc,
    arsrc, arbuf, stsrc, stbuf, dsrc, dbuf, tsrc, tbuf, rowd,
    l_s, xa_s, xa_r, ga_s, ga_r, ag_s, ag_r, cn_s, cn_r, ar_s, ar_r, st_s, st_r,
    d_s, d_r, t_s, t_r, rs_s, rs_r, o_s, o_r,
):
    n, ns, rows, sub, half, width = dims
    q = n * sub
    layers = ns
    j = lax.axis_index("dp")
    s = lax.axis_index("section")
    t = lax.axis_index("tensor")
    up, down, other = lax.rem(j + 1, n), lax.rem(j + n - 1, n), 1 - t
    pending = []

    def remote(src, dst, send, recv, device):
        return pltpu.make_async_remote_copy(
            src_ref=src, dst_ref=dst, send_sem=send, recv_sem=recv,
            device_id=device, device_id_type=MESH,
        )

    def go(*args):
        copy = remote(*args)
        copy.start()
        pending.append(copy)
        return copy

    def block(offset):
        return lax.rem(j + n + offset, n)

    part = [pl.ds(0, half), pl.ds(half, half)]
    owned = [vown, oown]
    locals_ = [
        pltpu.make_async_copy(hid, xfull.at[pl.ds(0, rows)], l_s.at[0]),
        pltpu.make_async_copy(une, xfull.at[pl.ds(rows, rows)], l_s.at[1]),
        pltpu.make_async_copy(vown.at[s], wfull.at[s, j, :, part[0]], l_s.at[2]),
        pltpu.make_async_copy(oown.at[s], wfull.at[s, j, :, part[1]], l_s.at[3]),
    ]
    for copy in reversed(locals_):
        copy.start()

    barrier = pltpu.get_barrier_semaphore()
    peers = [{"dp": up}, {"dp": down}, {"tensor": other}]
    peers += [{"section": lax.rem(s + k, ns)} for k in range(1, ns)]
    for peer in peers:
        pl.semaphore_signal(barrier, inc=1, device_id=peer, device_id_type=MESH)

    resp, pos = lens.shape[1], ref_t.shape[0]
    row_index = lax.broadcasted_iota(jnp.int32, (rows, resp), 0)
    lane_index = lax.broadcasted_iota(jnp.int32, (rows, resp), 1)
    offset = row_index - lane_index * pos
    mine = (offset >= 0) & (offset < pos)

    def spread(values):
        if values.shape[0] == pos:
            values = jnp.concatenate([values] * resp, axis=0)
        return jnp.sum(jnp.where(mine, values, 0.0), axis=1, keepdims=True)

    response = spread(lane_index.astype(F32))
    held = jnp.max(
        jnp.where(assign[...].astype(F32) == response, 1.0, 0.0), axis=1, keepdims=True
    )
    live = jnp.sum(jnp.where(mine & (offset < lens[...]), 1.0, 0.0), axis=1, keepdims=True)
    adv_col = spread(adv[...])
    gap_col = spread(gap_t[...])
    clipped = (adv_col > 0) & (gap_col > clip_high) | (adv_col < 0) & (gap_col < clip_low)
    rowd[0] = jnp.broadcast_to(
        jnp.where(clipped, 0.0, -loss_scale * adv_col * live * held), (rows, 128)
    )
    rowd[1] = jnp.broadcast_to(spread(ref_t[...]), (rows, 128))
    rowd[2] = jnp.broadcast_to(held, (rows, 128))
    gbuf[s] = gown[...]
    tokens_here = jnp.sum((surv[...] * lens[...]).astype(F32), axis=1, keepdims=True)
    cnts[j] = jnp.broadcast_to(tokens_here, cnts.shape[1:])

    pl.semaphore_wait(barrier, len(peers))

    def hand_out():
        for k in range(1, ns):
            to = lax.rem(s + k, ns)
            for p in range(2):
                remote(
                    owned[p].at[to], wfull.at[s, j, :, part[p]],
                    xa_s.at[p, k - 1], xa_r.at[p, s], {"section": to},
                ).start()

    for k in range(1, ns):
        to = lax.rem(s + k, ns)
        go(gown, gbuf.at[s], ga_s.at[k - 1], ga_r.at[s], {"section": to})
        for p in range(2):
            pending.append(
                remote(
                    owned[p].at[to], wfull.at[s, j, :, part[p]],
                    xa_s.at[p, k - 1], xa_r.at[p, s], {"section": to},
                )
            )
    pl.when(s < 2)(hand_out)
    for copy in locals_[2:]:
        copy.wait()

    def layer_arrived(l):
        @pl.when(s != l)
        def _():
            away = {"section": lax.rem(s + 1, ns)}
            for p in range(2):
                remote(owned[p].at[0], wfull.at[l, j, :, part[p]], xa_s.at[p, 0], xa_r.at[p, l], away).wait_recv()

    steps = n // 2

    def reach(l, p, way):
        return steps if (l + p + way) % 2 == 0 else steps - 1

    toward = [{"dp": up}, {"dp": down}]
    sign = [1, -1]

    def ag_copy(l, p, k, way, b):
        piece = wfull.at[l, b, :, part[p]]
        at = (l, p, way, k - 1)
        return (piece, piece, ag_s.at[at], ag_r.at[at], toward[way])

    def cn_copy(k, way, b):
        return (cnts.at[b], cnts.at[b], cn_s.at[way, k - 1], cn_r.at[way, k - 1], toward[way])

    def ag_send(l, p, k, way):
        if k <= reach(l, p, way):
            b = block(-sign[way] * (k - 1))
            go(*ag_copy(l, p, k, way, b))
            if l == 0 and p == 0:
                go(*cn_copy(k, way, b))

    def ag_recv(l, p, k, way):
        if k <= reach(l, p, way):
            b = block(-sign[way] * k)
            remote(*ag_copy(l, p, k, way, b)).wait_recv()
            if l == 0 and p == 0:
                remote(*cn_copy(k, way, b)).wait_recv()

    def ag_tick(ls, k):
        for l in ls:
            for p in range(2):
                for way in range(2):
                    ag_recv(l, p, k, way)
                    ag_send(l, p, k + 1, way)

    def ag_start(l):
        layer_arrived(l)
        for p in range(2):
            for way in range(2):
                ag_send(l, p, 1, way)

    eye = lax.broadcasted_iota(jnp.int32, (rows, rows), 0) == lax.broadcasted_iota(jnp.int32, (rows, rows), 1)

    def to_row(column):
        return jnp.sum(jnp.where(eye, column, 0.0), axis=0, keepdims=True)

    def to_col(row):
        return jnp.sum(jnp.where(eye, row, 0.0), axis=1, keepdims=True)

    def weight(l, first):
        w = wfull[l, :, :, 0:half] if first else wfull[l, :, :, half : 2 * half]
        return w.reshape(q, half)

    def gain(l):
        return gall[l : l + 1, :]

    def ar_send(i, value, stats=None):
        arsrc[i] = value
        if stats is not None:
            first = lax.broadcasted_iota(jnp.int32, (8, rows), 0) == 0
            stsrc[i] = jnp.where(first, stats[0], stats[1])
        for k in range(1, ns):
            to = {"section": lax.rem(s + k, ns)}
            if stats is not None:
                go(stsrc.at[i], stbuf.at[i, k - 1], st_s.at[i, k - 1], st_r.at[i, k - 1], to)
            go(arsrc.at[i], arbuf.at[i, k - 1], ar_s.at[i, k - 1], ar_r.at[i, k - 1], to)

    def ar_recv(i, stats=False):
        away = {"section": lax.rem(s + 1, ns)}
        if stats:
            for k in range(1, ns):
                remote(stsrc.at[i], stbuf.at[i, k - 1], st_s.at[i, k - 1], st_r.at[i, k - 1], away).wait_recv()
            both = stsrc[i]
            for k in range(1, ns):
                both = both + stbuf[i, k - 1]
        for k in range(1, ns):
            remote(arsrc.at[i], arbuf.at[i, k - 1], ar_s.at[i, k - 1], ar_r.at[i, k - 1], away).wait_recv()
        total = arsrc[i].astype(F32)
        for k in range(1, ns):
            total = total + arbuf[i, k - 1].astype(F32)
        return (total, both) if stats else total

    def pair_send(i, value):
        dsrc[i] = value
        go(dsrc.at[i], dbuf.at[i], d_s.at[i], d_r.at[i], {"tensor": other})

    def pair_recv(i):
        remote(dsrc.at[i], dbuf.at[i], d_s.at[i], d_r.at[i], {"tensor": other}).wait_recv()
        return dsrc[i].astype(F32) + dbuf[i].astype(F32)

    def small_send(i, column):
        tsrc[i] = jnp.broadcast_to(to_row(column), (8, rows))
        go(tsrc.at[i], tbuf.at[i], t_s.at[i], t_r.at[i], {"tensor": other})

    def small_recv(i):
        remote(tsrc.at[i], tbuf.at[i], t_s.at[i], t_r.at[i], {"tensor": other}).wait_recv()
        return to_col(tsrc[i, 0:1, :] + tbuf[i, 0:1, :])

    def select_features():
        for l in range(layers):
            @pl.when(s != l)
            def _():
                away = {"section": lax.rem(s + 1, ns)}
                remote(gown, gbuf.at[l], ga_s.at[0], ga_r.at[l], away).wait_recv()
        gains = gbuf[:, 0, :]
        high = gains.astype(BF16).astype(F32)
        middle = (gains - high).astype(BF16).astype(F32)
        low = gains - high - middle
        pad = jnp.zeros((16 - 3 * layers, width), F32)
        xfull[2 * rows :, :] = jnp.concatenate([high, middle, low, pad], axis=0).astype(BF16)
        for copy in locals_[:2]:
            copy.wait()
        size = math.lcm(sub, 128)
        place = lax.broadcasted_iota(jnp.int32, (size, size), 0)
        lane = lax.broadcasted_iota(jnp.int32, (size, size), 1)
        slices = jnp.zeros((size, size), jnp.int32)
        for m in range(1, size // sub):
            slices = slices + (lane >= m * sub).astype(jnp.int32)
        target = lane + slices * ((ns - 1) * sub) + s * sub
        for super_index in range(width // (ns * size)):
            total = None
            for c in range(ns):
                pick = (place + c * size == target).astype(F32).astype(BF16)
                at = (super_index * ns + c) * size
                piece = dot_nn(xfull[:, at : at + size], pick)
                total = piece if total is None else total + piece
            span = slice(super_index * size, (super_index + 1) * size)
            xs[0, :, span] = total[:rows].astype(BF16)
            us[:, span] = total[rows : 2 * rows].astype(BF16)
            parts = total[2 * rows : 2 * rows + 16]
            gall[:, span] = parts[:layers] + parts[layers : 2 * layers] + parts[2 * layers : 3 * layers]

    def contribute(l):
        x = xs[l].astype(F32)
        xg = (x * gain(l)).astype(BF16)
        partial = dot_nn(xg, weight(l, True)).astype(BF16)
        squares = to_row(jnp.sum(x * x, axis=1, keepdims=True))
        inner = squares
        if l == layers - 1:
            inner = to_row(jnp.sum(x * us[...].astype(F32), axis=1, keepdims=True))
        ar_send(l, partial, (squares, inner))

    def collect(l):
        total, both = ar_recv(l, True)
        inverse = lax.rsqrt(to_col(both[0:1, :]) / width + eps_norm)
        rcols[l] = jnp.broadcast_to(inverse, (rows, 128))
        projs[l] = (total * inverse).astype(BF16)
        return both[1:2, :]

    def mix(l):
        pair_send(l, dot_nt(projs[l], weight(l, False)).astype(BF16))

    def advance(l):
        xs[l + 1] = (xs[l].astype(F32) + pair_recv(l)).astype(BF16)

    def early():
        contribute(0)
        yield
        collect(0)
        mix(0)
        yield
        advance(0)
        contribute(1)
        yield
        collect(1)
        mix(1)
        yield
        advance(1)
        yield

    for l in (0, 1):
        ag_start(l)
    pl.when(s >= 2)(hand_out)
    select_features()
    for k in range(1, steps + 1):
        ag_tick((0, 1), k)
        if k == steps:
            for l in (2, 3):
                ag_start(l)
    stage = early()
    for k in range(1, steps + 1):
        next(stage, None)
        ag_tick((2, 3), k)
    for _ in stage:
        pass

    contribute(2)
    ar_send(4, dot_nn(us[...], weight(3, False)).astype(BF16))
    collect(2)
    mix(2)
    advance(2)
    contribute(3)
    inner_row = collect(3)
    top = ar_recv(4)
    small_send(3, jnp.sum(projs[3].astype(F32) * top, axis=1, keepdims=True))

    def wgrad(l, gp):
        normed = (xs[l].astype(F32) * rcols[l, :, 0:1] * gain(l)).astype(BF16)
        wg[l, :, :, 0:half] = dot_tn(normed, gp).astype(BF16).reshape(n, sub, half)
        wg[l, :, :, half : 2 * half] = dot_tn(gcur[...], projs[l]).astype(BF16).reshape(n, sub, half)

    landing = [rbu, rbd]

    def rs_copy(l, p, i, way, b):
        at = (l, p, way, i - 1)
        return (
            wg.at[l, b, :, part[p]], landing[way].at[l, i - 1, :, part[p]],
            rs_s.at[at], rs_r.at[at], toward[way],
        )

    def rs_send(l, p, i, way):
        hops = reach(l, p, way)
        if i <= hops:
            go(*rs_copy(l, p, i, way, block(sign[way] * (hops - i + 1))))

    def rs_recv(l, p, i, way):
        hops = reach(l, p, way)
        if i <= hops:
            b = block(sign[way] * (hops - i))
            remote(*rs_copy(l, p, i, way, b)).wait_recv()
            cols = slice(p * half, (p + 1) * half)
            wg[l, b, :, cols] = (
                wg[l, b, :, cols].astype(F32) + landing[way][l, i - 1, :, cols].astype(F32)
            ).astype(BF16)

    position = {}

    def rs_start(l):
        for p in range(2):
            for way in range(2):
                rs_send(l, p, 1, way)
        position[l] = 1

    def rs_tick():
        for l in sorted(position, reverse=True):
            i = position[l]
            if i > steps:
                continue
            for p in range(2):
                for way in range(2):
                    rs_recv(l, p, i, way)
                    rs_send(l, p, i + 1, way)
            position[l] = i + 1
            if i == steps:
                finish(l)

    def finish(l):
        osrc[l] = wg[l, j]

        @pl.when(s == l)
        def _():
            obuf[l] = osrc[l]

        @pl.when(s != l)
        def _():
            remote(osrc.at[l], obuf.at[s], o_s.at[l], o_r.at[s], {"section": l}).start()

    wcol, base, held = rowd[0, :, 0:1], rowd[1, :, 0:1], rowd[2, :, 0:1]
    inner = to_col(inner_row)
    logit = inner + small_recv(3)
    seed = wcol * jnp.exp(jnp.where(held > 0.0, logit - base, 0.0))
    gp = (seed * top).astype(BF16)
    gcur[...] = (seed * us[...].astype(F32)).astype(BF16)
    for l in range(layers - 1, 0, -1):
        pair_send(2 + l, dot_nt(gp, weight(l, True)).astype(BF16))
        small_send(l - 1, jnp.sum(gp.astype(F32) * projs[l].astype(F32), axis=1, keepdims=True))
        wgrad(l, gp)
        rs_start(l)
        if l < layers - 1:
            rs_tick()
        grad_normed = pair_recv(2 + l)
        inverse = rcols[l, :, 0:1]
        inner = small_recv(l - 1) * (inverse * inverse) / width
        gcur[...] = (
            gcur[...].astype(F32) + inverse * gain(l) * grad_normed - xs[l].astype(F32) * inner
        ).astype(BF16)
        ar_send(4 + l, dot_nn(gcur[...], weight(l - 1, False)).astype(BF16))
        rs_tick()
        rs_tick()
        gp = ar_recv(4 + l).astype(BF16)
    wgrad(0, gp)
    rs_start(0)
    while any(i <= steps for i in position.values()):
        rs_tick()

    for l in range(layers):
        @pl.when(s != l)
        def _():
            remote(osrc.at[l], obuf.at[l], o_s.at[l], o_r.at[l], {"section": l}).wait_send()
            remote(osrc.at[l], obuf.at[l], o_s.at[l], o_r.at[l], {"section": l}).wait_recv()
    tokens = jnp.sum(cnts[:, 0:1, 0:1])
    out[...] = obuf[...].astype(F32) / tokens
    for copy in pending:
        copy.wait_send()


def local(
    hidden,
    unembed,
    value_proj,
    output_proj,
    norm_gains,
    survive,
    lengths,
    assign,
    advantage,
    reference_logit,
    recorded_gap,
):
    resp_count, positions, width = hidden.shape
    own, half = value_proj.shape[1:]
    n, ns = lax.axis_size("dp"), lax.axis_size("section")
    rows = resp_count * positions
    sub = own // ns
    q = n * sub
    dims = (n, ns, rows, sub, half, width)
    steps = n // 2
    vmem = pl.BlockSpec(memory_space=pltpu.VMEM)
    anywhere = pl.BlockSpec(memory_space=pl.ANY)
    dma = pltpu.SemaphoreType.DMA
    out = pl.pallas_call(
        functools.partial(kernel, dims),
        out_shape=jax.ShapeDtypeStruct((ns, sub, 2 * half), F32),
        in_specs=[anywhere] * 4 + [vmem] * 7,
        out_specs=vmem,
        scratch_shapes=[
            pltpu.VMEM((2 * rows + 16, width), BF16),
            pltpu.VMEM((ns, 1, width), F32),
            pltpu.VMEM((ns, n, sub, 2 * half), BF16),
            pltpu.VMEM((ns, q), F32),
            pltpu.VMEM((n, 8, rows), F32),
            pltpu.VMEM((ns, rows, q), BF16),
            pltpu.VMEM((rows, q), BF16),
            pltpu.VMEM((ns, rows, half), BF16),
            pltpu.VMEM((ns, rows, 128), F32),
            pltpu.VMEM((rows, q), BF16),
            pltpu.VMEM((ns, n, sub, 2 * half), BF16),
            pltpu.VMEM((ns, steps, sub, 2 * half), BF16),
            pltpu.VMEM((ns, steps, sub, 2 * half), BF16),
            pltpu.VMEM((ns, sub, 2 * half), BF16),
            pltpu.VMEM((ns, sub, 2 * half), BF16),
            pltpu.VMEM((8, rows, half), BF16),
            pltpu.VMEM((8, ns - 1, rows, half), BF16),
            pltpu.VMEM((ns, 8, rows), F32),
            pltpu.VMEM((ns, ns - 1, 8, rows), F32),
            pltpu.VMEM((6, rows, q), BF16),
            pltpu.VMEM((6, rows, q), BF16),
            pltpu.VMEM((4, 8, rows), F32),
            pltpu.VMEM((4, 8, rows), F32),
            pltpu.VMEM((3, rows, 128), F32),
            dma((4,)), dma((2, ns - 1)), dma((2, ns)), dma((ns - 1,)), dma((ns,)),
            dma((ns, 2, 2, steps)), dma((ns, 2, 2, steps)), dma((2, steps)), dma((2, steps)),
            dma((8, ns - 1)), dma((8, ns - 1)), dma((ns, ns - 1)), dma((ns, ns - 1)),
            dma((6,)), dma((6,)), dma((4,)), dma((4,)),
            dma((ns, 2, 2, steps)), dma((ns, 2, 2, steps)), dma((ns,)), dma((ns,)),
        ],
        compiler_params=pltpu.CompilerParams(
            collective_id=0, has_side_effects=True, vmem_limit_bytes=60 * 1024 * 1024
        ),
    )(
        hidden.reshape(rows, width),
        unembed.reshape(rows, width),
        value_proj.reshape(ns, sub, half),
        output_proj[0].T.reshape(ns, sub, half),
        norm_gains,
        survive.reshape(1, 1),
        lengths.reshape(1, resp_count),
        assign.reshape(1, resp_count),
        advantage.reshape(1, resp_count),
        reference_logit.T,
        recorded_gap.T,
    )
    flat = out.reshape(own, 2 * half)
    return (flat[:, :half][None], flat[:, half:].T[None])


def solution(mesh):
    placed = (
        P(("groups", "dp"), None, None),
        P(("groups", "dp"), None, None),
        P("section", "dp", "tensor"),
        P("section", "tensor", "dp"),
        P("section", None),
        P(("groups", "dp")),
        P(("groups", "dp")),
        P(("groups", "dp")),
        P(("groups", "dp")),
        P(("groups", "dp"), None),
        P(("groups", "dp"), None),
    )
    return jax.shard_map(
        local,
        mesh=mesh,
        in_specs=placed,
        out_specs=(
            P(("groups", "section"), "dp", "tensor"),
            P(("groups", "section"), "tensor", "dp"),
        ),
        check_vma=False,
    )
```

```python
import functools
import math

import jax
import jax.numpy as jnp
from jax import lax
from jax.experimental import pallas as pl
from jax.experimental.pallas import tpu as pltpu
from jax.sharding import PartitionSpec as P

eps_norm = 1e-06
loss_scale = 4096.0
clip_high = math.log(1.28)
clip_low = math.log(0.8)

F32 = jnp.float32
BF16 = jnp.bfloat16
MESH = pl.DeviceIdType.MESH

RING_START = (0, 0, 5, 8)
CHAIN_AT = (8, 10, 13, 16)
RING_STEPS = ((0, 1), (0, 1), (0, 1))


def dot_nn(a, b):
    return jnp.dot(a, b, preferred_element_type=F32)


def dot_nt(a, b):
    return lax.dot_general(a, b, (((1,), (1,)), ((), ())), preferred_element_type=F32)


def dot_tn(a, b):
    return lax.dot_general(a, b, (((0,), (0,)), ((), ())), preferred_element_type=F32)


def kernel(
    dims,
    hid, une, vown, oown, gown, surv, lens, assign, adv, ref_t, gap_t,
    out,
    xfull, gbuf, wfull, wpeer, gall, cnts, xs, us, projs, rcols, wg, rbu, rbd, obuf, osrc,
    arsrc, arbuf, stsrc, stbuf, nrows, grows, prows, qrows, psrc, qsrc, rowd, picks,
    l_s, xa_s, xa_r, ga_s, ga_r, ag_s, ag_r, cn_s, cn_r, ar_s, ar_r, st_s, st_r,
    pw_s, pw_r, ex_s, ex_r, rs_s, rs_r, o_s, o_r,
):
    n, ns, rows, sub, half, width = dims
    q = n * sub
    layers = ns
    mine_rows = rows // 2
    j = lax.axis_index("dp")
    s = lax.axis_index("section")
    t = lax.axis_index("tensor")
    up, down, other = lax.rem(j + 1, n), lax.rem(j + n - 1, n), 1 - t
    pending = []

    def remote(src, dst, send, recv, device):
        return pltpu.make_async_remote_copy(
            src_ref=src, dst_ref=dst, send_sem=send, recv_sem=recv,
            device_id=device, device_id_type=MESH,
        )

    def go(*args):
        copy = remote(*args)
        copy.start()
        pending.append(copy)
        return copy

    def block(offset):
        return lax.rem(j + n + offset, n)

    part = [pl.ds(0, half), pl.ds(half, half)]
    owned = [vown, oown]
    locals_ = [
        pltpu.make_async_copy(hid.at[t], xfull.at[pl.ds(0, mine_rows)], l_s.at[0]),
        pltpu.make_async_copy(une.at[t], xfull.at[pl.ds(mine_rows, mine_rows)], l_s.at[1]),
        pltpu.make_async_copy(vown.at[s], wfull.at[s, j, :, part[0]], l_s.at[2]),
        pltpu.make_async_copy(oown.at[s], wfull.at[s, j, :, part[1]], l_s.at[3]),
    ]
    for copy in reversed(locals_):
        copy.start()

    barrier = pltpu.get_barrier_semaphore()
    peers = [{"dp": up}, {"dp": down}, {"tensor": other}]
    peers += [{"section": lax.rem(s + k, ns)} for k in range(1, ns)]
    for peer in peers:
        pl.semaphore_signal(barrier, inc=1, device_id=peer, device_id_type=MESH)

    resp, pos = lens.shape[1], ref_t.shape[0]
    row_index = lax.broadcasted_iota(jnp.int32, (mine_rows, resp), 0) + t * mine_rows
    lane_index = lax.broadcasted_iota(jnp.int32, (mine_rows, resp), 1)
    offset = row_index - lane_index * pos
    mine = (offset >= 0) & (offset < pos)

    def spread(values):
        if values.shape[0] == pos:
            values = jnp.concatenate([values] * (mine_rows // pos), axis=0)
        return jnp.sum(jnp.where(mine, values, 0.0), axis=1, keepdims=True)

    response = spread(lane_index.astype(F32))
    held = jnp.max(
        jnp.where(assign[...].astype(F32) == response, 1.0, 0.0), axis=1, keepdims=True
    )
    live = jnp.sum(jnp.where(mine & (offset < lens[...]), 1.0, 0.0), axis=1, keepdims=True)
    adv_col = spread(adv[...])
    gap_col = spread(gap_t[...])
    clipped = (adv_col > 0) & (gap_col > clip_high) | (adv_col < 0) & (gap_col < clip_low)
    rowd[0] = jnp.broadcast_to(
        jnp.where(clipped, 0.0, -loss_scale * adv_col * live * held), (mine_rows, 128)
    )
    rowd[1] = jnp.broadcast_to(spread(ref_t[...]), (mine_rows, 128))
    rowd[2] = jnp.broadcast_to(held, (mine_rows, 128))
    gbuf[s] = gown[...]
    tokens_here = jnp.sum((surv[...] * lens[...]).astype(F32), axis=1, keepdims=True)
    cnts[j] = jnp.broadcast_to(tokens_here, cnts.shape[1:])

    pl.semaphore_wait(barrier, len(peers))

    def hand_out():
        for k in range(1, ns):
            to = lax.rem(s + k, ns)
            for p in range(2):
                remote(
                    owned[p].at[to], wfull.at[s, j, :, part[p]],
                    xa_s.at[p, k - 1], xa_r.at[p, s], {"section": to},
                ).start()

    for k in range(1, ns):
        to = lax.rem(s + k, ns)
        go(gown, gbuf.at[s], ga_s.at[k - 1], ga_r.at[s], {"section": to})
        for p in range(2):
            pending.append(
                remote(
                    owned[p].at[to], wfull.at[s, j, :, part[p]],
                    xa_s.at[p, k - 1], xa_r.at[p, s], {"section": to},
                )
            )
    pl.when(s < 2)(hand_out)
    for copy in locals_[2:]:
        copy.wait()

    def layer_arrived(l):
        @pl.when(s != l)
        def _():
            away = {"section": lax.rem(s + 1, ns)}
            for p in range(2):
                remote(owned[p].at[0], wfull.at[l, j, :, part[p]], xa_s.at[p, 0], xa_r.at[p, l], away).wait_recv()

    steps = n // 2

    def reach(l, p, way):
        return steps if (l + p + way) % 2 == 0 else steps - 1

    toward = [{"dp": up}, {"dp": down}]
    sign = [1, -1]

    def ag_copy(l, p, k, way, b):
        piece = wfull.at[l, b, :, part[p]]
        at = (l, p, way, k - 1)
        return (piece, piece, ag_s.at[at], ag_r.at[at], toward[way])

    def cn_copy(k, way, b):
        return (cnts.at[b], cnts.at[b], cn_s.at[way, k - 1], cn_r.at[way, k - 1], toward[way])

    def ag_send(l, p, k, way):
        if k <= reach(l, p, way):
            b = block(-sign[way] * (k - 1))
            go(*ag_copy(l, p, k, way, b))
            if l == 0 and p == 0:
                go(*cn_copy(k, way, b))

    def ag_recv(l, p, k, way):
        if k <= reach(l, p, way):
            b = block(-sign[way] * k)
            remote(*ag_copy(l, p, k, way, b)).wait_recv()
            if l == 0 and p == 0:
                remote(*cn_copy(k, way, b)).wait_recv()

    def peer_copy(l, slot, b):
        return (wfull.at[l, b], wpeer.at[l, b], pw_s.at[l, slot], pw_r.at[l, slot], {"tensor": other})

    def peer_arrived(l):
        remote(*peer_copy(l, 0, j)).wait_recv()
        for slot in range(1, n):
            remote(*peer_copy(l, slot, j)).wait_recv()

    def ag_tick(tick):
        for l in range(layers):
            k = tick - RING_START[l]
            if 1 <= k <= steps:
                for p in range(2):
                    for way in range(2):
                        ag_recv(l, p, k, way)
                        ag_send(l, p, k + 1, way)
                go(*peer_copy(l, 2 * k - 1, block(-k)))
                if k < steps:
                    go(*peer_copy(l, 2 * k, block(k)))

    def ag_start(l):
        layer_arrived(l)
        for p in range(2):
            for way in range(2):
                ag_send(l, p, 1, way)
        go(*peer_copy(l, 0, j))

    eye = lax.broadcasted_iota(jnp.int32, (mine_rows, 128), 0) == lax.broadcasted_iota(jnp.int32, (mine_rows, 128), 1)

    def to_row(column):
        return jnp.sum(jnp.where(eye, column, 0.0), axis=0, keepdims=True)

    def to_col(row):
        return jnp.sum(jnp.where(eye, row, 0.0), axis=1, keepdims=True)

    def forward_dot(rows_in, l, which):
        cols = slice(which * half, (which + 1) * half)
        return jnp.concatenate(
            [dot_nn(rows_in, w[l, :, :, cols].reshape(q, half)) for w in (wfull, wpeer)], axis=1
        )

    def backward_dot(rows_in, l, which):
        cols = slice(which * half, (which + 1) * half)
        return dot_nt(rows_in[:, :half], wfull[l, :, :, cols].reshape(q, half)) + dot_nt(
            rows_in[:, half:], wpeer[l, :, :, cols].reshape(q, half)
        )

    def gain(l):
        return gall[l : l + 1, :]

    def ar_send(i, value, stats=None):
        arsrc[i] = value
        if stats is not None:
            first = lax.broadcasted_iota(jnp.int32, (8, 128), 0) == 0
            stsrc[i] = jnp.where(first, stats[0], stats[1])
        for k in range(1, ns):
            to = {"section": lax.rem(s + k, ns)}
            if stats is not None:
                go(stsrc.at[i], stbuf.at[i, k - 1], st_s.at[i, k - 1], st_r.at[i, k - 1], to)
            go(arsrc.at[i], arbuf.at[i, k - 1], ar_s.at[i, k - 1], ar_r.at[i, k - 1], to)

    def ar_recv(i, stats=False):
        away = {"section": lax.rem(s + 1, ns)}
        if stats:
            for k in range(1, ns):
                remote(stsrc.at[i], stbuf.at[i, k - 1], st_s.at[i, k - 1], st_r.at[i, k - 1], away).wait_recv()
            both = stsrc[i]
            for k in range(1, ns):
                both = both + stbuf[i, k - 1]
        for k in range(1, ns):
            remote(arsrc.at[i], arbuf.at[i, k - 1], ar_s.at[i, k - 1], ar_r.at[i, k - 1], away).wait_recv()
        total = arsrc[i].astype(F32)
        for k in range(1, ns):
            total = total + arbuf[i, k - 1].astype(F32)
        return (total, both) if stats else total

    def swap_copy(kind, l):
        held_rows = (nrows, grows)[kind] if kind < 2 else (prows, qrows)[kind - 2]
        source = held_rows.at[l, pl.ds(0, mine_rows)] if kind < 2 else (psrc, qsrc)[kind - 2].at[l]
        return (
            source, held_rows.at[l, pl.ds(mine_rows, mine_rows)],
            ex_s.at[kind, l], ex_r.at[kind, l], {"tensor": other},
        )

    def swap(kind, l, value):
        if kind < 2:
            (nrows, grows)[kind][l, 0:mine_rows] = value
        else:
            (prows, qrows)[kind - 2][l, 0:mine_rows] = value[:, :half]
            (psrc, qsrc)[kind - 2][l] = value[:, half:]
        go(*swap_copy(kind, l))

    def swapped(kind, l):
        remote(*swap_copy(kind, l)).wait_recv()

    def select_features():
        size = math.lcm(sub, 128)
        place = lax.broadcasted_iota(jnp.int32, (size, size), 0)
        lane = lax.broadcasted_iota(jnp.int32, (size, size), 1)
        slices = jnp.zeros((size, size), jnp.int32)
        for m in range(1, size // sub):
            slices = slices + (lane >= m * sub).astype(jnp.int32)
        target = lane + slices * ((ns - 1) * sub) + s * sub - place
        for c in range(ns):
            picks[c] = (target == c * size).astype(F32).astype(BF16)
        for l in range(layers):
            @pl.when(s != l)
            def _():
                away = {"section": lax.rem(s + 1, ns)}
                remote(gown, gbuf.at[l], ga_s.at[0], ga_r.at[l], away).wait_recv()
        gains = gbuf[:, 0, :]
        high = gains.astype(BF16).astype(F32)
        middle = (gains - high).astype(BF16).astype(F32)
        low = gains - high - middle
        pad = jnp.zeros((16 - 3 * layers, width), F32)
        xfull[2 * mine_rows :, :] = jnp.concatenate([high, middle, low, pad], axis=0).astype(BF16)
        for copy in locals_[:2]:
            copy.wait()
        for super_index in range(width // (ns * size)):
            total = None
            for c in range(ns):
                at = (super_index * ns + c) * size
                piece = dot_nn(xfull[:, at : at + size], picks[c])
                total = piece if total is None else total + piece
            span = slice(super_index * size, (super_index + 1) * size)
            xs[0, :, span] = total[:mine_rows].astype(BF16)
            us[:, span] = total[mine_rows : 2 * mine_rows].astype(BF16)
            parts = total[2 * mine_rows : 2 * mine_rows + 16]
            gall[:, span] = parts[:layers] + parts[layers : 2 * layers] + parts[2 * layers : 3 * layers]

    def contribute(l):
        peer_arrived(l)
        x = xs[l].astype(F32)
        xg = (x * gain(l)).astype(BF16)
        partial = forward_dot(xg, l, 0).astype(BF16)
        squares = to_row(jnp.sum(x * x, axis=1, keepdims=True))
        inner = squares
        if l == layers - 1:
            inner = to_row(jnp.sum(x * us[...].astype(F32), axis=1, keepdims=True))
        ar_send(l, partial, (squares, inner))

    def collect(l):
        total, both = ar_recv(l, True)
        inverse = lax.rsqrt(to_col(both[0:1, :]) / width + eps_norm)
        rcols[l] = jnp.broadcast_to(inverse, (mine_rows, 128))
        proj = (total * inverse).astype(BF16)
        projs[l] = proj
        if l < layers - 1:
            mixed = backward_dot(proj, l, 1)
            xs[l + 1] = (xs[l].astype(F32) + mixed).astype(BF16)
        return both[1:2, :]

    def share(l):
        swap(0, l, (xs[l].astype(F32) * rcols[l, :, 0:1] * gain(l)).astype(BF16))
        swap(2, l, projs[l])

    def chain():
        contribute(0)
        yield
        collect(0)
        contribute(1)
        share(0)
        yield
        collect(1)
        contribute(2)
        share(1)
        yield
        collect(2)
        contribute(3)
        ar_send(4, forward_dot(us[...], 3, 1).astype(BF16))
        share(2)
        yield

    stage = chain()
    for tick in range(max(RING_START) + steps + 1):
        if tick > 0:
            ag_tick(tick)
        for l in range(layers):
            if tick == RING_START[l]:
                ag_start(l)
        if tick == 0:
            pl.when(s >= 2)(hand_out)
            select_features()
        for _ in range(CHAIN_AT.count(tick)):
            next(stage)
    for _ in stage:
        pass
    inner_row = collect(3)
    top = ar_recv(4)
    share(3)

    def wgrad_value(l):
        swapped(0, l)
        swapped(3, l)
        wg[l, :, :, 0:half] = dot_tn(nrows[l], qrows[l]).astype(BF16).reshape(n, sub, half)
        rs_start(l, 0)

    def wgrad_output(l):
        swapped(1, l)
        swapped(2, l)
        wg[l, :, :, half : 2 * half] = dot_tn(grows[l], prows[l]).astype(BF16).reshape(n, sub, half)
        rs_start(l, 1)

    landing = [rbu, rbd]

    def rs_copy(l, p, i, way, b):
        at = (l, p, way, i - 1)
        return (
            wg.at[l, b, :, part[p]], landing[way].at[l, i - 1, :, part[p]],
            rs_s.at[at], rs_r.at[at], toward[way],
        )

    def rs_send(l, p, i, way):
        hops = reach(l, p, way)
        if i <= hops:
            go(*rs_copy(l, p, i, way, block(sign[way] * (hops - i + 1))))

    def rs_recv(l, p, i, way):
        hops = reach(l, p, way)
        if i <= hops:
            b = block(sign[way] * (hops - i))
            remote(*rs_copy(l, p, i, way, b)).wait_recv()
            cols = slice(p * half, (p + 1) * half)
            wg[l, b, :, cols] = (
                wg[l, b, :, cols].astype(F32) + landing[way][l, i - 1, :, cols].astype(F32)
            ).astype(BF16)

    position = {}

    def rs_start(l, p):
        for way in range(2):
            rs_send(l, p, 1, way)
        position[l, p] = 1

    def rs_tick():
        for l, p in sorted(position, reverse=True):
            i = position[l, p]
            if i > steps:
                continue
            for way in range(2):
                rs_recv(l, p, i, way)
                rs_send(l, p, i + 1, way)
            position[l, p] = i + 1
            if i == steps and position.get((l, 1 - p), 0) > steps:
                finish(l)

    def rs_ticks(count):
        for _ in range(count):
            rs_tick()

    def finish(l):
        osrc[l] = wg[l, j]

        @pl.when(s == l)
        def _():
            obuf[l] = osrc[l]

        @pl.when(s != l)
        def _():
            remote(osrc.at[l], obuf.at[s], o_s.at[l], o_r.at[s], {"section": l}).start()

    wcol, base, held = rowd[0, :, 0:1], rowd[1, :, 0:1], rowd[2, :, 0:1]
    inner = to_col(inner_row)
    logit = inner + jnp.sum(projs[3].astype(F32) * top, axis=1, keepdims=True)
    seed = wcol * jnp.exp(jnp.where(held > 0.0, logit - base, 0.0))
    upstream = (seed * us[...].astype(F32)).astype(BF16)
    gp = (seed * top).astype(BF16)
    swap(1, layers - 1, upstream)
    for l in range(layers - 1, 0, -1):
        turns = RING_STEPS[layers - 1 - l]
        swap(3, l, gp)
        grad_normed = backward_dot(gp, l, 0)
        inverse = rcols[l, :, 0:1]
        inner = jnp.sum(gp.astype(F32) * projs[l].astype(F32), axis=1, keepdims=True)
        inner = inner * (inverse * inverse) / width
        upstream = (
            upstream.astype(F32) + inverse * gain(l) * grad_normed - xs[l].astype(F32) * inner
        ).astype(BF16)
        ar_send(4 + l, forward_dot(upstream, l - 1, 1).astype(BF16))
        swap(1, l - 1, upstream)
        if l == layers - 1:
            wgrad_output(l)
        wgrad_value(l)
        rs_ticks(turns[0])
        wgrad_output(l - 1)
        rs_ticks(turns[1])
        gp = ar_recv(4 + l).astype(BF16)
    swap(3, 0, gp)
    rs_ticks(1)
    wgrad_value(0)
    while any(i <= steps for i in position.values()):
        rs_tick()

    for l in range(layers):
        @pl.when(s != l)
        def _():
            remote(osrc.at[l], obuf.at[l], o_s.at[l], o_r.at[l], {"section": l}).wait_send()
            remote(osrc.at[l], obuf.at[l], o_s.at[l], o_r.at[l], {"section": l}).wait_recv()
    tokens = jnp.sum(cnts[:, 0:1, 0:1])
    out[...] = obuf[...].astype(F32) / tokens
    for copy in pending:
        copy.wait_send()


def local(
    hidden,
    unembed,
    value_proj,
    output_proj,
    norm_gains,
    survive,
    lengths,
    assign,
    advantage,
    reference_logit,
    recorded_gap,
):
    resp_count, positions, width = hidden.shape
    own, half = value_proj.shape[1:]
    n, ns = lax.axis_size("dp"), lax.axis_size("section")
    rows = resp_count * positions
    sub = own // ns
    q = n * sub
    dims = (n, ns, rows, sub, half, width)
    steps = n // 2
    vmem = pl.BlockSpec(memory_space=pltpu.VMEM)
    anywhere = pl.BlockSpec(memory_space=pl.ANY)
    dma = pltpu.SemaphoreType.DMA
    out = pl.pallas_call(
        functools.partial(kernel, dims),
        out_shape=jax.ShapeDtypeStruct((ns, sub, 2 * half), F32),
        in_specs=[anywhere] * 4 + [vmem] * 7,
        out_specs=vmem,
        scratch_shapes=[
            pltpu.VMEM((rows + 16, width), BF16),
            pltpu.VMEM((ns, 1, width), F32),
            pltpu.VMEM((ns, n, sub, 2 * half), BF16),
            pltpu.VMEM((ns, n, sub, 2 * half), BF16),
            pltpu.VMEM((ns, q), F32),
            pltpu.VMEM((n, 8, 128), F32),
            pltpu.VMEM((ns, rows // 2, q), BF16),
            pltpu.VMEM((rows // 2, q), BF16),
            pltpu.VMEM((ns, rows // 2, 2 * half), BF16),
            pltpu.VMEM((ns, rows // 2, 128), F32),
            pltpu.VMEM((ns, n, sub, 2 * half), BF16),
            pltpu.VMEM((ns, steps, sub, 2 * half), BF16),
            pltpu.VMEM((ns, steps, sub, 2 * half), BF16),
            pltpu.VMEM((ns, sub, 2 * half), BF16),
            pltpu.VMEM((ns, sub, 2 * half), BF16),
            pltpu.VMEM((8, rows // 2, 2 * half), BF16),
            pltpu.VMEM((8, ns - 1, rows // 2, 2 * half), BF16),
            pltpu.VMEM((ns, 8, 128), F32),
            pltpu.VMEM((ns, ns - 1, 8, 128), F32),
            pltpu.VMEM((ns, rows, q), BF16),
            pltpu.VMEM((ns, rows, q), BF16),
            pltpu.VMEM((ns, rows, half), BF16),
            pltpu.VMEM((ns, rows, half), BF16),
            pltpu.VMEM((ns, rows // 2, half), BF16),
            pltpu.VMEM((ns, rows // 2, half), BF16),
            pltpu.VMEM((3, rows // 2, 128), F32),
            pltpu.VMEM((ns, math.lcm(sub, 128), math.lcm(sub, 128)), BF16),
            dma((4,)), dma((2, ns - 1)), dma((2, ns)), dma((ns - 1,)), dma((ns,)),
            dma((ns, 2, 2, steps)), dma((ns, 2, 2, steps)), dma((2, steps)), dma((2, steps)),
            dma((8, ns - 1)), dma((8, ns - 1)), dma((ns, ns - 1)), dma((ns, ns - 1)),
            dma((ns, n)), dma((ns, n)), dma((4, ns)), dma((4, ns)),
            dma((ns, 2, 2, steps)), dma((ns, 2, 2, steps)), dma((ns,)), dma((ns,)),
        ],
        compiler_params=pltpu.CompilerParams(
            collective_id=0, has_side_effects=True, vmem_limit_bytes=60 * 1024 * 1024
        ),
    )(
        hidden.reshape(2, rows // 2, width),
        unembed.reshape(2, rows // 2, width),
        value_proj.reshape(ns, sub, half),
        output_proj[0].T.reshape(ns, sub, half),
        norm_gains,
        survive.reshape(1, 1),
        lengths.reshape(1, resp_count),
        assign.reshape(1, resp_count),
        advantage.reshape(1, resp_count),
        reference_logit.T,
        recorded_gap.T,
    )
    flat = out.reshape(own, 2 * half)
    return (flat[:, :half][None], flat[:, half:].T[None])


def solution(mesh):
    placed = (
        P(("groups", "dp"), None, None),
        P(("groups", "dp"), None, None),
        P("section", "dp", "tensor"),
        P("section", "tensor", "dp"),
        P("section", None),
        P(("groups", "dp")),
        P(("groups", "dp")),
        P(("groups", "dp")),
        P(("groups", "dp")),
        P(("groups", "dp"), None),
        P(("groups", "dp"), None),
    )
    return jax.shard_map(
        local,
        mesh=mesh,
        in_specs=placed,
        out_specs=(
            P(("groups", "section"), "dp", "tensor"),
            P(("groups", "section"), "tensor", "dp"),
        ),
        check_vma=False,
    )
```

```python
import functools
import math

import jax
import jax.numpy as jnp
from jax import lax
from jax.experimental import pallas as pl
from jax.experimental.pallas import tpu as pltpu
from jax.sharding import PartitionSpec as P

eps_norm = 1e-06
loss_scale = 4096.0
clip_high = math.log(1.28)
clip_low = math.log(0.8)

F32 = jnp.float32
BF16 = jnp.bfloat16
MESH = pl.DeviceIdType.MESH

RING_START = (0, 0, 5, 8)
CHAIN_AT = (8, 10, 13, 16)
RING_STEPS = ((0, 1), (0, 1), (0, 1))


def dot_nn(a, b):
    return jnp.dot(a, b, preferred_element_type=F32)


def dot_nt(a, b):
    return lax.dot_general(a, b, (((1,), (1,)), ((), ())), preferred_element_type=F32)


def dot_tn(a, b):
    return lax.dot_general(a, b, (((0,), (0,)), ((), ())), preferred_element_type=F32)


def kernel(
    dims,
    hid, une, vown, oown, gown, surv, lens, assign, adv, ref_t, gap_t,
    out,
    xfull, gbuf, wfull, wpeer, gall, cnts, xs, us, projs, rcols, wg, rbu, rbd, obuf, osrc,
    arsrc, arbuf, stsrc, stbuf, nrows, grows, prows, qrows, psrc, qsrc, rowd, picks,
    l_s, xa_s, xa_r, ga_s, ga_r, ag_s, ag_r, cn_s, cn_r, ar_s, ar_r, st_s, st_r,
    pw_s, pw_r, ex_s, ex_r, rs_s, rs_r, o_s, o_r,
):
    n, ns, rows, sub, half, width = dims
    q = n * sub
    layers = ns
    mine_rows = rows // 2
    j = lax.axis_index("dp")
    s = lax.axis_index("section")
    t = lax.axis_index("tensor")
    up, down, other = lax.rem(j + 1, n), lax.rem(j + n - 1, n), 1 - t
    pending = []

    def remote(src, dst, send, recv, device):
        return pltpu.make_async_remote_copy(
            src_ref=src, dst_ref=dst, send_sem=send, recv_sem=recv,
            device_id=device, device_id_type=MESH,
        )

    def go(*args):
        copy = remote(*args)
        copy.start()
        pending.append(copy)
        return copy

    def block(offset):
        return lax.rem(j + n + offset, n)

    part = [pl.ds(0, half), pl.ds(half, half)]
    owned = [vown, oown]
    locals_ = [
        pltpu.make_async_copy(hid.at[t], xfull.at[pl.ds(0, mine_rows)], l_s.at[0]),
        pltpu.make_async_copy(une.at[t], xfull.at[pl.ds(mine_rows, mine_rows)], l_s.at[1]),
        pltpu.make_async_copy(vown.at[s], wfull.at[s, j, :, part[0]], l_s.at[2]),
        pltpu.make_async_copy(oown.at[s], wfull.at[s, j, :, part[1]], l_s.at[3]),
    ]
    for copy in reversed(locals_):
        copy.start()

    barrier = pltpu.get_barrier_semaphore()
    peers = [{"dp": up}, {"dp": down}, {"tensor": other}]
    peers += [{"section": lax.rem(s + k, ns)} for k in range(1, ns)]
    for peer in peers:
        pl.semaphore_signal(barrier, inc=1, device_id=peer, device_id_type=MESH)

    resp, pos = lens.shape[1], ref_t.shape[0]
    row_index = lax.broadcasted_iota(jnp.int32, (mine_rows, resp), 0) + t * mine_rows
    lane_index = lax.broadcasted_iota(jnp.int32, (mine_rows, resp), 1)
    offset = row_index - lane_index * pos
    mine = (offset >= 0) & (offset < pos)

    def spread(values):
        if values.shape[0] == pos:
            values = jnp.concatenate([values] * (mine_rows // pos), axis=0)
        return jnp.sum(jnp.where(mine, values, 0.0), axis=1, keepdims=True)

    response = spread(lane_index.astype(F32))
    held = jnp.max(
        jnp.where(assign[...].astype(F32) == response, 1.0, 0.0), axis=1, keepdims=True
    )
    live = jnp.sum(jnp.where(mine & (offset < lens[...]), 1.0, 0.0), axis=1, keepdims=True)
    adv_col = spread(adv[...])
    gap_col = spread(gap_t[...])
    clipped = (adv_col > 0) & (gap_col > clip_high) | (adv_col < 0) & (gap_col < clip_low)
    rowd[0] = jnp.broadcast_to(
        jnp.where(clipped, 0.0, -loss_scale * adv_col * live * held), (mine_rows, 128)
    )
    rowd[1] = jnp.broadcast_to(spread(ref_t[...]), (mine_rows, 128))
    rowd[2] = jnp.broadcast_to(held, (mine_rows, 128))
    gbuf[s] = gown[...]
    tokens_here = jnp.sum((surv[...] * lens[...]).astype(F32), axis=1, keepdims=True)
    cnts[j] = jnp.broadcast_to(tokens_here, cnts.shape[1:])

    pl.semaphore_wait(barrier, len(peers))

    def hand_out():
        for k in range(1, ns):
            to = lax.rem(s + k, ns)
            for p in range(2):
                remote(
                    owned[p].at[to], wfull.at[s, j, :, part[p]],
                    xa_s.at[p, k - 1], xa_r.at[p, s], {"section": to},
                ).start()

    for k in range(1, ns):
        to = lax.rem(s + k, ns)
        go(gown, gbuf.at[s], ga_s.at[k - 1], ga_r.at[s], {"section": to})
        for p in range(2):
            pending.append(
                remote(
                    owned[p].at[to], wfull.at[s, j, :, part[p]],
                    xa_s.at[p, k - 1], xa_r.at[p, s], {"section": to},
                )
            )
    pl.when(s < 2)(hand_out)
    for copy in locals_[2:]:
        copy.wait()

    def layer_arrived(l):
        @pl.when(s != l)
        def _():
            away = {"section": lax.rem(s + 1, ns)}
            for p in range(2):
                remote(owned[p].at[0], wfull.at[l, j, :, part[p]], xa_s.at[p, 0], xa_r.at[p, l], away).wait_recv()

    steps = n // 2

    def reach(l, p, way):
        return steps if (l + p + way) % 2 == 0 else steps - 1

    toward = [{"dp": up}, {"dp": down}]
    sign = [1, -1]

    def ag_copy(l, p, k, way, b):
        piece = wfull.at[l, b, :, part[p]]
        at = (l, p, way, k - 1)
        return (piece, piece, ag_s.at[at], ag_r.at[at], toward[way])

    def cn_copy(k, way, b):
        return (cnts.at[b], cnts.at[b], cn_s.at[way, k - 1], cn_r.at[way, k - 1], toward[way])

    def ag_send(l, p, k, way):
        if k <= reach(l, p, way):
            b = block(-sign[way] * (k - 1))
            go(*ag_copy(l, p, k, way, b))
            if l == 0 and p == 0:
                go(*cn_copy(k, way, b))

    def ag_recv(l, p, k, way):
        if k <= reach(l, p, way):
            b = block(-sign[way] * k)
            remote(*ag_copy(l, p, k, way, b)).wait_recv()
            if l == 0 and p == 0:
                remote(*cn_copy(k, way, b)).wait_recv()

    def peer_copy(l, slot, b):
        return (wfull.at[l, b], wpeer.at[l, b], pw_s.at[l, slot], pw_r.at[l, slot], {"tensor": other})

    def peer_arrived(l):
        remote(*peer_copy(l, 0, j)).wait_recv()
        for slot in range(1, n):
            remote(*peer_copy(l, slot, j)).wait_recv()

    def ag_tick(tick):
        for l in range(layers):
            k = tick - RING_START[l]
            if 1 <= k <= steps:
                for p in range(2):
                    for way in range(2):
                        ag_recv(l, p, k, way)
                        ag_send(l, p, k + 1, way)
                go(*peer_copy(l, 2 * k - 1, block(-k)))
                if k < steps:
                    go(*peer_copy(l, 2 * k, block(k)))

    def ag_start(l):
        layer_arrived(l)
        for p in range(2):
            for way in range(2):
                ag_send(l, p, 1, way)
        go(*peer_copy(l, 0, j))

    eye = lax.broadcasted_iota(jnp.int32, (mine_rows, 128), 0) == lax.broadcasted_iota(jnp.int32, (mine_rows, 128), 1)

    def to_row(column):
        return jnp.sum(jnp.where(eye, column, 0.0), axis=0, keepdims=True)

    def to_col(row):
        return jnp.sum(jnp.where(eye, row, 0.0), axis=1, keepdims=True)

    def forward_dot(rows_in, l, which):
        cols = slice(which * half, (which + 1) * half)
        return jnp.concatenate(
            [dot_nn(rows_in, w[l, :, :, cols].reshape(q, half)) for w in (wfull, wpeer)], axis=1
        )

    def backward_dot(rows_in, l, which):
        cols = slice(which * half, (which + 1) * half)
        return dot_nt(rows_in[:, :half], wfull[l, :, :, cols].reshape(q, half)) + dot_nt(
            rows_in[:, half:], wpeer[l, :, :, cols].reshape(q, half)
        )

    def gain(l):
        return gall[l : l + 1, :]

    def ar_send(i, value, stats=None):
        arsrc[i] = value
        if stats is not None:
            first = lax.broadcasted_iota(jnp.int32, (8, 128), 0) == 0
            stsrc[i] = jnp.where(first, stats[0], stats[1])
        for k in range(1, ns):
            to = {"section": lax.rem(s + k, ns)}
            if stats is not None:
                go(stsrc.at[i], stbuf.at[i, k - 1], st_s.at[i, k - 1], st_r.at[i, k - 1], to)
            go(arsrc.at[i], arbuf.at[i, k - 1], ar_s.at[i, k - 1], ar_r.at[i, k - 1], to)

    def ar_recv(i, stats=False):
        away = {"section": lax.rem(s + 1, ns)}
        if stats:
            for k in range(1, ns):
                remote(stsrc.at[i], stbuf.at[i, k - 1], st_s.at[i, k - 1], st_r.at[i, k - 1], away).wait_recv()
            both = stsrc[i]
            for k in range(1, ns):
                both = both + stbuf[i, k - 1]
        for k in range(1, ns):
            remote(arsrc.at[i], arbuf.at[i, k - 1], ar_s.at[i, k - 1], ar_r.at[i, k - 1], away).wait_recv()
        total = arsrc[i].astype(F32)
        for k in range(1, ns):
            total = total + arbuf[i, k - 1].astype(F32)
        return (total, both) if stats else total

    def swap_copy(kind, l):
        held_rows = (nrows, grows)[kind] if kind < 2 else (prows, qrows)[kind - 2]
        source = held_rows.at[l, pl.ds(0, mine_rows)] if kind < 2 else (psrc, qsrc)[kind - 2].at[l]
        return (
            source, held_rows.at[l, pl.ds(mine_rows, mine_rows)],
            ex_s.at[kind, l], ex_r.at[kind, l], {"tensor": other},
        )

    def swap(kind, l, value):
        if kind < 2:
            (nrows, grows)[kind][l, 0:mine_rows] = value
        else:
            (prows, qrows)[kind - 2][l, 0:mine_rows] = value[:, :half]
            (psrc, qsrc)[kind - 2][l] = value[:, half:]
        go(*swap_copy(kind, l))

    def swapped(kind, l):
        remote(*swap_copy(kind, l)).wait_recv()

    def select_features():
        size = math.lcm(sub, 128)
        place = lax.broadcasted_iota(jnp.int32, (size, size), 0)
        lane = lax.broadcasted_iota(jnp.int32, (size, size), 1)
        slices = jnp.zeros((size, size), jnp.int32)
        for m in range(1, size // sub):
            slices = slices + (lane >= m * sub).astype(jnp.int32)
        target = lane + slices * ((ns - 1) * sub) + s * sub - place
        for c in range(ns):
            picks[c] = (target == c * size).astype(F32).astype(BF16)
        for l in range(layers):
            @pl.when(s != l)
            def _():
                away = {"section": lax.rem(s + 1, ns)}
                remote(gown, gbuf.at[l], ga_s.at[0], ga_r.at[l], away).wait_recv()
        gains = gbuf[:, 0, :]
        high = gains.astype(BF16).astype(F32)
        middle = (gains - high).astype(BF16).astype(F32)
        low = gains - high - middle
        pad = jnp.zeros((16 - 3 * layers, width), F32)
        xfull[2 * mine_rows :, :] = jnp.concatenate([high, middle, low, pad], axis=0).astype(BF16)
        for copy in locals_[:2]:
            copy.wait()
        for super_index in range(width // (ns * size)):
            total = None
            for c in range(ns):
                at = (super_index * ns + c) * size
                piece = dot_nn(xfull[:, at : at + size], picks[c])
                total = piece if total is None else total + piece
            span = slice(super_index * size, (super_index + 1) * size)
            xs[0, :, span] = total[:mine_rows].astype(BF16)
            us[:, span] = total[mine_rows : 2 * mine_rows].astype(BF16)
            parts = total[2 * mine_rows : 2 * mine_rows + 16]
            gall[:, span] = parts[:layers] + parts[layers : 2 * layers] + parts[2 * layers : 3 * layers]

    def contribute(l):
        peer_arrived(l)
        x = xs[l].astype(F32)
        xg = (x * gain(l)).astype(BF16)
        partial = forward_dot(xg, l, 0).astype(BF16)
        squares = to_row(jnp.sum(x * x, axis=1, keepdims=True))
        inner = squares
        if l == layers - 1:
            inner = to_row(jnp.sum(x * us[...].astype(F32), axis=1, keepdims=True))
        ar_send(l, partial, (squares, inner))

    def collect(l):
        total, both = ar_recv(l, True)
        inverse = lax.rsqrt(to_col(both[0:1, :]) / width + eps_norm)
        rcols[l] = jnp.broadcast_to(inverse, (mine_rows, 128))
        proj = (total * inverse).astype(BF16)
        projs[l] = proj
        if l < layers - 1:
            mixed = backward_dot(proj, l, 1)
            xs[l + 1] = (xs[l].astype(F32) + mixed).astype(BF16)
        return both[1:2, :]

    def share(l):
        swap(0, l, (xs[l].astype(F32) * rcols[l, :, 0:1] * gain(l)).astype(BF16))
        swap(2, l, projs[l])

    def chain():
        contribute(0)
        yield
        collect(0)
        contribute(1)
        share(0)
        yield
        collect(1)
        contribute(2)
        share(1)
        yield
        collect(2)
        contribute(3)
        ar_send(4, forward_dot(us[...], 3, 1).astype(BF16))
        share(2)
        yield

    stage = chain()
    for tick in range(max(RING_START) + steps + 1):
        if tick > 0:
            ag_tick(tick)
        for l in range(layers):
            if tick == RING_START[l]:
                ag_start(l)
        if tick == 0:
            pl.when(s >= 2)(hand_out)
            select_features()
        for _ in range(CHAIN_AT.count(tick)):
            next(stage)
    for _ in stage:
        pass
    inner_row = collect(3)
    top = ar_recv(4)
    share(3)

    def wgrad_value(l):
        swapped(0, l)
        swapped(3, l)
        wg[l, :, :, 0:half] = dot_tn(nrows[l], qrows[l]).astype(BF16).reshape(n, sub, half)
        rs_start(l, 0)

    def wgrad_output(l):
        swapped(1, l)
        swapped(2, l)
        wg[l, :, :, half : 2 * half] = dot_tn(grows[l], prows[l]).astype(BF16).reshape(n, sub, half)
        rs_start(l, 1)

    landing = [rbu, rbd]

    def rs_copy(l, p, i, way, b):
        at = (l, p, way, i - 1)
        return (
            wg.at[l, b, :, part[p]], landing[way].at[l, i - 1, :, part[p]],
            rs_s.at[at], rs_r.at[at], toward[way],
        )

    def rs_send(l, p, i, way):
        hops = reach(l, p, way)
        if i <= hops:
            go(*rs_copy(l, p, i, way, block(sign[way] * (hops - i + 1))))

    def rs_recv(l, p, i, way):
        hops = reach(l, p, way)
        if i <= hops:
            b = block(sign[way] * (hops - i))
            remote(*rs_copy(l, p, i, way, b)).wait_recv()
            cols = slice(p * half, (p + 1) * half)
            wg[l, b, :, cols] = (
                wg[l, b, :, cols].astype(F32) + landing[way][l, i - 1, :, cols].astype(F32)
            ).astype(BF16)

    position = {}

    def rs_start(l, p):
        for way in range(2):
            rs_send(l, p, 1, way)
        position[l, p] = 1

    def rs_tick():
        for l, p in sorted(position, reverse=True):
            i = position[l, p]
            if i > steps:
                continue
            for way in range(2):
                rs_recv(l, p, i, way)
                rs_send(l, p, i + 1, way)
            position[l, p] = i + 1
            if i == steps and position.get((l, 1 - p), 0) > steps:
                finish(l)

    def rs_ticks(count):
        for _ in range(count):
            rs_tick()

    def finish(l):
        osrc[l] = wg[l, j]

        @pl.when(s == l)
        def _():
            obuf[l] = osrc[l]

        @pl.when(s != l)
        def _():
            remote(osrc.at[l], obuf.at[s], o_s.at[l], o_r.at[s], {"section": l}).start()

    wcol, base, held = rowd[0, :, 0:1], rowd[1, :, 0:1], rowd[2, :, 0:1]
    inner = to_col(inner_row)
    logit = inner + jnp.sum(projs[3].astype(F32) * top, axis=1, keepdims=True)
    seed = wcol * jnp.exp(jnp.where(held > 0.0, logit - base, 0.0))
    upstream = (seed * us[...].astype(F32)).astype(BF16)
    gp = (seed * top).astype(BF16)
    swap(1, layers - 1, upstream)
    for l in range(layers - 1, 0, -1):
        turns = RING_STEPS[layers - 1 - l]
        swap(3, l, gp)
        grad_normed = backward_dot(gp, l, 0)
        if l == layers - 1:
            wgrad_output(l)
            wgrad_value(l)
        inverse = rcols[l, :, 0:1]
        inner = jnp.sum(gp.astype(F32) * projs[l].astype(F32), axis=1, keepdims=True)
        inner = inner * (inverse * inverse) / width
        upstream = (
            upstream.astype(F32) + inverse * gain(l) * grad_normed - xs[l].astype(F32) * inner
        ).astype(BF16)
        ar_send(4 + l, forward_dot(upstream, l - 1, 1).astype(BF16))
        swap(1, l - 1, upstream)
        if l < layers - 1:
            wgrad_value(l)
        rs_ticks(turns[0])
        wgrad_output(l - 1)
        rs_ticks(turns[1])
        gp = ar_recv(4 + l).astype(BF16)
    swap(3, 0, gp)
    rs_ticks(1)
    wgrad_value(0)
    while any(i <= steps for i in position.values()):
        rs_tick()

    for l in range(layers):
        @pl.when(s != l)
        def _():
            remote(osrc.at[l], obuf.at[l], o_s.at[l], o_r.at[l], {"section": l}).wait_send()
            remote(osrc.at[l], obuf.at[l], o_s.at[l], o_r.at[l], {"section": l}).wait_recv()
    tokens = jnp.sum(cnts[:, 0:1, 0:1])
    out[...] = obuf[...].astype(F32) / tokens
    for copy in pending:
        copy.wait_send()


def local(
    hidden,
    unembed,
    value_proj,
    output_proj,
    norm_gains,
    survive,
    lengths,
    assign,
    advantage,
    reference_logit,
    recorded_gap,
):
    resp_count, positions, width = hidden.shape
    own, half = value_proj.shape[1:]
    n, ns = lax.axis_size("dp"), lax.axis_size("section")
    rows = resp_count * positions
    sub = own // ns
    q = n * sub
    dims = (n, ns, rows, sub, half, width)
    steps = n // 2
    vmem = pl.BlockSpec(memory_space=pltpu.VMEM)
    anywhere = pl.BlockSpec(memory_space=pl.ANY)
    dma = pltpu.SemaphoreType.DMA
    out = pl.pallas_call(
        functools.partial(kernel, dims),
        out_shape=jax.ShapeDtypeStruct((ns, sub, 2 * half), F32),
        in_specs=[anywhere] * 4 + [vmem] * 7,
        out_specs=vmem,
        scratch_shapes=[
            pltpu.VMEM((rows + 16, width), BF16),
            pltpu.VMEM((ns, 1, width), F32),
            pltpu.VMEM((ns, n, sub, 2 * half), BF16),
            pltpu.VMEM((ns, n, sub, 2 * half), BF16),
            pltpu.VMEM((ns, q), F32),
            pltpu.VMEM((n, 8, 128), F32),
            pltpu.VMEM((ns, rows // 2, q), BF16),
            pltpu.VMEM((rows // 2, q), BF16),
            pltpu.VMEM((ns, rows // 2, 2 * half), BF16),
            pltpu.VMEM((ns, rows // 2, 128), F32),
            pltpu.VMEM((ns, n, sub, 2 * half), BF16),
            pltpu.VMEM((ns, steps, sub, 2 * half), BF16),
            pltpu.VMEM((ns, steps, sub, 2 * half), BF16),
            pltpu.VMEM((ns, sub, 2 * half), BF16),
            pltpu.VMEM((ns, sub, 2 * half), BF16),
            pltpu.VMEM((8, rows // 2, 2 * half), BF16),
            pltpu.VMEM((8, ns - 1, rows // 2, 2 * half), BF16),
            pltpu.VMEM((ns, 8, 128), F32),
            pltpu.VMEM((ns, ns - 1, 8, 128), F32),
            pltpu.VMEM((ns, rows, q), BF16),
            pltpu.VMEM((ns, rows, q), BF16),
            pltpu.VMEM((ns, rows, half), BF16),
            pltpu.VMEM((ns, rows, half), BF16),
            pltpu.VMEM((ns, rows // 2, half), BF16),
            pltpu.VMEM((ns, rows // 2, half), BF16),
            pltpu.VMEM((3, rows // 2, 128), F32),
            pltpu.VMEM((ns, math.lcm(sub, 128), math.lcm(sub, 128)), BF16),
            dma((4,)), dma((2, ns - 1)), dma((2, ns)), dma((ns - 1,)), dma((ns,)),
            dma((ns, 2, 2, steps)), dma((ns, 2, 2, steps)), dma((2, steps)), dma((2, steps)),
            dma((8, ns - 1)), dma((8, ns - 1)), dma((ns, ns - 1)), dma((ns, ns - 1)),
            dma((ns, n)), dma((ns, n)), dma((4, ns)), dma((4, ns)),
            dma((ns, 2, 2, steps)), dma((ns, 2, 2, steps)), dma((ns,)), dma((ns,)),
        ],
        compiler_params=pltpu.CompilerParams(
            collective_id=0, has_side_effects=True, vmem_limit_bytes=60 * 1024 * 1024
        ),
    )(
        hidden.reshape(2, rows // 2, width),
        unembed.reshape(2, rows // 2, width),
        value_proj.reshape(ns, sub, half),
        output_proj[0].T.reshape(ns, sub, half),
        norm_gains,
        survive.reshape(1, 1),
        lengths.reshape(1, resp_count),
        assign.reshape(1, resp_count),
        advantage.reshape(1, resp_count),
        reference_logit.T,
        recorded_gap.T,
    )
    flat = out.reshape(own, 2 * half)
    return (flat[:, :half][None], flat[:, half:].T[None])


def solution(mesh):
    placed = (
        P(("groups", "dp"), None, None),
        P(("groups", "dp"), None, None),
        P("section", "dp", "tensor"),
        P("section", "tensor", "dp"),
        P("section", None),
        P(("groups", "dp")),
        P(("groups", "dp")),
        P(("groups", "dp")),
        P(("groups", "dp")),
        P(("groups", "dp"), None),
        P(("groups", "dp"), None),
    )
    return jax.shard_map(
        local,
        mesh=mesh,
        in_specs=placed,
        out_specs=(
            P(("groups", "section"), "dp", "tensor"),
            P(("groups", "section"), "tensor", "dp"),
        ),
        check_vma=False,
    )
```
